512 devices in a mesh: cand: 8 (over x, core), blk: 8 (over z), feat: 8 (over y).
Axes of the slice: x: 4, y: 8, z: 8, core: 2. Of those that a mesh axis runs over, the one named last changes fastest.
Arguments:
- embeddings: float32 [131072, 1024], P(('cand', 'blk'), 'feat'), may hold values from -12 to 12
- winners: int32 [32, 3], replicated, may hold values from 0 to 131071, as said below
Outputs:
- columns: float32 [32, 3, 131072], P(None, None, ('cand', 'blk'))
- gains: float32 [32, 131072], P(None, ('cand', 'blk'))
- best: float32 [32, 3], replicated
The draws below stay inside these ranges and needn't reach their ends.
Inputs may be any that keep to these rules, and one draw needn't show every extreme that they name: winners[b,k] lies in [k * 43690, (k + 1) * 43690), so the winners of a session are distinct.
All inputs are finite; a program needn't handle non-finite values.
Results may differ from the reference program's by a relative error of at most 0.00012.
Values sent between devices are 32-bit elements; how exact they have to be, the bound alone decides.
No kernel may reach another device: no remote copies, remote signals or barrier semaphores. Data moves between devices by JAX's collectives and lax.ppermute only.
A program may use at most 64 MiB of HBM per device.

```python
import math
import jax
import jax.numpy as jnp
from jax import lax

D = 1024
SESSIONS = 32
STEPS = 3
CANDS = 131072


def pick_winners(key):
    third = CANDS // STEPS
    picks = jax.random.randint(key, (SESSIONS, STEPS), 0, third)
    offsets = jnp.arange(STEPS, dtype=jnp.int32) * third
    return (picks + offsets[None, :]).astype(jnp.int32)


def draw_winners(key, part):
    return pick_winners(jax.random.fold_in(key, 11))


def draw_embeddings(key, part):
    chosen = pick_winners(jax.random.fold_in(key, 11))
    key_rows = jax.random.fold_in(key, 21)
    key_scale = jax.random.fold_in(key, 22)
    drawn = jnp.clip(jax.random.normal(key_rows, (CANDS, D), jnp.float32), -6.0, 6.0)
    scale = jnp.exp(jax.random.uniform(key_scale, (CANDS,), jnp.float32, math.log(0.2), math.log(2.0)))
    sessions = jnp.arange(SESSIONS, dtype=jnp.int32)
    step_index = jnp.arange(STEPS, dtype=jnp.int32)
    low_step = 1 + sessions // 2 % (STEPS - 1)
    forced = (sessions[:, None] % 2 == 1) & (step_index[None, :] == low_step[:, None])
    winner_scale = jnp.where(forced, 0.2, 1.0).astype(jnp.float32)
    flat = chosen.reshape(SESSIONS * STEPS)
    scale = scale.at[flat].set(1.0)
    scale = scale.at[flat].min(winner_scale.reshape(SESSIONS * STEPS))
    return (drawn * scale[:, None]).astype(jnp.float32)


def setup_inputs(seed: int = 0) -> dict:
    keys = jax.random.split(jax.random.key(seed), 3)
    embeddings = draw_embeddings(jax.random.fold_in(keys[2], 71), 0)
    winners = draw_winners(jax.random.fold_in(keys[2], 71), 0)
    return {"embeddings": embeddings, "winners": winners}


def reference(embeddings, winners):
    gains0 = lax.optimization_barrier(jnp.sum(embeddings * embeddings, axis=1)) / D
    gains = jnp.broadcast_to(gains0[None, :], (SESSIONS, CANDS)).astype(jnp.float32)
    columns = jnp.zeros((SESSIONS, STEPS, CANDS), jnp.float32)
    best_list = []
    for k in range(STEPS):
        best_list.append(lax.optimization_barrier(jnp.max(gains, axis=1)))
        chosen = winners[:, k].astype(jnp.int32)
        rows = embeddings[chosen]
        inner = jnp.dot(rows, embeddings.T, precision=lax.Precision.HIGHEST, preferred_element_type=jnp.float32) / D
        c_at = jnp.take_along_axis(columns, chosen[:, None, None], axis=2)[:, :, 0]
        d_at = jnp.take_along_axis(gains, chosen[:, None], axis=1)[:, 0]
        carried = jnp.einsum('bs,bsn->bn', c_at, columns, precision=lax.Precision.HIGHEST)
        update = (inner - carried) / jnp.sqrt(jnp.maximum(d_at, 0.1))[:, None]
        columns = columns.at[:, k, :].set(update)
        gains = gains - update * update
    return (columns, gains, jnp.stack(best_list, axis=1))
```

```python
import jax
import jax.numpy as jnp
from jax import lax
from jax.experimental import pallas as pl
from jax.experimental.pallas import tpu as pltpu
from jax.sharding import Mesh
from jax.sharding import PartitionSpec as P

D = 1024
CANDS = 131072
SESSIONS = 32
STEPS = 3
LANES = 128
PICKS = STEPS * SESSIONS
FLOOR = 0.1
CAND = ("cand_0", "cand_1")
CAND_BLK = ("cand_0", "cand_1", "blk")
FEAT = ("feat_hi", "feat_lo")
EXACT = lax.Precision.HIGHEST
PAIRS = [(t, u) for t in range(STEPS) for u in range(t, STEPS)]
VMEM = pl.BlockSpec(memory_space=pltpu.VMEM)


def share_with(array, axes):
    devices = lax.axis_size(axes)
    copies = jnp.broadcast_to(array, (devices, *array.shape))
    return lax.all_to_all(copies, axes, 0, 0, tiled=True)


def first_step(group, groups):
    return min(group * (CANDS // groups) // (CANDS // STEPS), STEPS - 2)


def winner_rows(embeddings, winners):
    rows_here, width = embeddings.shape
    groups = lax.axis_size(CAND)
    turn = [first_step(g, groups) for g in range(groups)].index(1)
    late = lax.axis_index(CAND) >= turn
    offset = lax.axis_index(CAND_BLK) * rows_here
    by_step = winners.T
    chosen = jnp.where(late, by_step[1:], by_step[:2]).reshape(2 * SESSIONS)
    positions = offset + jnp.arange(rows_here, dtype=jnp.int32)
    onehot = (positions[None, :] == chosen[:, None]).astype(jnp.float32)
    part = jnp.dot(onehot, embeddings, precision=EXACT, preferred_element_type=jnp.float32)
    group_rows = jnp.sum(share_with(part, "blk"), axis=0)
    spread = share_with(group_rows, (*CAND, "feat_lo"))
    spread = spread.reshape(groups, 2, 2, SESSIONS, width)
    low = jnp.sum(spread[:turn], axis=0)
    high = jnp.sum(spread[turn:], axis=0)
    rows = jnp.stack([low[:, 0], low[:, 1] + high[:, 0], high[:, 1]], axis=1)
    return rows.reshape(2, PICKS, width)


def times_rows(left, right):
    return lax.dot_general(
        left, right, (((1,), (1,)), ((), ())), precision=EXACT, preferred_element_type=jnp.float32
    )


def in_rows(tiles):
    at = lax.broadcasted_iota(jnp.int32, (8, LANES), 0)
    tile = jnp.zeros((8, LANES), jnp.float32)
    for row, values in enumerate(tiles):
        tile = jnp.where(at == row, jnp.broadcast_to(values[:1], (8, LANES)), tile)
    return tile


def products_kernel(rows_ref, other_rows_ref, mine_ref, got_ref, out_ref):
    ones = jnp.ones((8, LANES), jnp.float32)
    rows, other_rows = rows_ref[...], other_rows_ref[...]
    crossed = jnp.concatenate(
        [
            rows[t * SESSIONS : (t + 1) * SESSIONS] * rows[u * SESSIONS : (u + 1) * SESSIONS]
            + other_rows[t * SESSIONS : (t + 1) * SESSIONS] * other_rows[u * SESSIONS : (u + 1) * SESSIONS]
            for t, u in PAIRS
        ]
        + [jnp.zeros((2 * LANES - len(PAIRS) * SESSIONS, LANES), jnp.float32)]
    )
    gram = times_rows(ones, crossed)
    for q in range(out_ref.shape[0]):
        norms = []
        for h in range(2):
            at = pl.ds((2 * q + h) * LANES, LANES)
            mine, got = mine_ref[at, :], got_ref[at, :]
            out_ref[q, pl.ds(h * PICKS, PICKS), :] = times_rows(rows, mine) + times_rows(other_rows, got)
            norms.append(times_rows(ones, mine * mine + got * got))
        out_ref[q, pl.ds(2 * PICKS, 8), :] = in_rows([*norms, gram[:, :LANES], gram[:, LANES:]])


def columns_kernel(parts_ref, out_ref):
    total = parts_ref[0]
    for q in range(1, parts_ref.shape[0]):
        total = total + parts_ref[q]
    total = total * (1.0 / D)
    session = lax.broadcasted_iota(jnp.int32, (SESSIONS, LANES), 0)
    lane = lax.broadcasted_iota(jnp.int32, (SESSIONS, LANES), 1)
    gram = {}
    for i, pair in enumerate(PAIRS):
        row = total[2 * PICKS + 2 + i // 4 : 2 * PICKS + 3 + i // 4]
        picked = jnp.where(lane == (i % 4) * SESSIONS + session, jnp.broadcast_to(row, session.shape), 0.0)
        gram[pair] = jnp.sum(picked, axis=1, keepdims=True)
    factor, radius = {}, []
    for k in range(STEPS):
        left = gram[k, k]
        for t in range(k):
            left = left - factor[t, k] * factor[t, k]
        radius.append(jnp.sqrt(jnp.maximum(left, FLOOR)))
        for u in range(k + 1, STEPS):
            rest = gram[k, u]
            for t in range(k):
                rest = rest - factor[t, k] * factor[t, u]
            factor[k, u] = rest / radius[k]
    blocks, norms, tops = [], [], [[], []]
    for h in range(2):
        norm = total[2 * PICKS + h : 2 * PICKS + h + 1]
        norms.append(norm)
        gains = jnp.broadcast_to(norm, (SESSIONS, LANES))
        columns = []
        for k in range(STEPS):
            start = h * PICKS + k * SESSIONS
            column = total[start : start + SESSIONS]
            for t in range(k):
                column = column - factor[t, k] * columns[t]
            column = column / radius[k]
            columns.append(column)
            if k < STEPS - 1:
                gains = gains - column * column
                tops[k].append(jnp.max(gains, axis=1, keepdims=True))
        blocks += columns
    first = jnp.max(jnp.maximum(norms[0], norms[1]), axis=1, keepdims=True)
    maxima = [jnp.broadcast_to(first, (SESSIONS, 1))] + [jnp.maximum(*pair) for pair in tops]
    best = jnp.zeros((1, LANES), jnp.float32)
    for k, values in enumerate(maxima):
        placed = jnp.where(lane == k * SESSIONS + session, jnp.broadcast_to(values, session.shape), 0.0)
        best = best + jnp.sum(placed, axis=0, keepdims=True)
    whole = jnp.concatenate([*blocks, in_rows([*norms, best])])
    for f in range(out_ref.shape[0]):
        out_ref[f] = whole


def results_kernel(spread_ref, columns_ref, gains_ref):
    his = spread_ref.shape[0] // 2
    for f in range(2 * his):
        for h in range(2):
            at = pl.ds(((f % 2) * his + f // 2) * 2 * LANES + h * LANES, LANES)
            gains = jnp.broadcast_to(spread_ref[f, pl.ds(2 * PICKS + h, 1), :], (SESSIONS, LANES))
            for k in range(STEPS):
                column = spread_ref[f, pl.ds(h * PICKS + k * SESSIONS, SESSIONS), :]
                columns_ref[k, :, at] = column
                gains = gains - column * column
            gains_ref[:, at] = gains


def selection(embeddings, winners):
    rows_here, _ = embeddings.shape
    his, half = lax.axis_size("feat_hi"), rows_here // 2
    side = lax.axis_index("feat_lo")
    mine = lax.dynamic_slice_in_dim(embeddings, side * half, half)
    other = lax.dynamic_slice_in_dim(embeddings, (1 - side) * half, half)
    got = lax.ppermute(other, "feat_lo", [(0, 1), (1, 0)])
    rows = winner_rows(embeddings, winners)
    own_rows = jnp.where(side == 0, rows[0], rows[1])
    other_rows = jnp.where(side == 0, rows[1], rows[0])
    piece = (2 * PICKS + 8, LANES)
    products = pl.pallas_call(
        products_kernel,
        out_shape=jax.ShapeDtypeStruct((his, *piece), jnp.float32),
        in_specs=[VMEM] * 4,
        out_specs=VMEM,
        cost_estimate=pl.CostEstimate(flops=2 * PICKS * half * 256, bytes_accessed=2 << 20, transcendentals=0),
    )(own_rows, other_rows, mine, got)
    parts = lax.all_to_all(products, "feat_hi", 0, 0, tiled=True)
    share = pl.pallas_call(
        columns_kernel,
        out_shape=jax.ShapeDtypeStruct((2 * his, *piece), jnp.float32),
        in_specs=[VMEM],
        out_specs=VMEM,
        cost_estimate=pl.CostEstimate(flops=1 << 20, bytes_accessed=2 << 20, transcendentals=0),
    )(parts)
    spread = lax.all_to_all(share, FEAT, 0, 0, tiled=True)
    tops = jnp.max(spread[:, 2 * PICKS + 2, :], axis=0)
    best = share_with(tops.reshape(1, LANES), CAND_BLK).max(axis=(0, 1))
    best = best[:PICKS].reshape(STEPS, SESSIONS).T
    columns, gains = pl.pallas_call(
        results_kernel,
        out_shape=(
            jax.ShapeDtypeStruct((STEPS, SESSIONS, rows_here), jnp.float32),
            jax.ShapeDtypeStruct((SESSIONS, rows_here), jnp.float32),
        ),
        in_specs=[VMEM],
        out_specs=(VMEM, VMEM),
        cost_estimate=pl.CostEstimate(flops=1 << 20, bytes_accessed=2 << 20, transcendentals=0),
    )(spread)
    return (columns.transpose(1, 0, 2), gains, best)


def solution(mesh):
    torus = Mesh(
        mesh.devices.reshape(4, 2, mesh.shape["blk"], mesh.shape["feat"] // 2, 2),
        ("cand_0", "cand_1", "blk", "feat_hi", "feat_lo"),
    )
    return jax.shard_map(
        selection,
        mesh=torus,
        in_specs=(P(CAND_BLK, FEAT), P()),
        out_specs=(P(None, None, CAND_BLK), P(None, CAND_BLK), P()),
        check_vma=False,
    )
```

```python
import jax
import jax.numpy as jnp
from jax import lax
from jax.experimental import pallas as pl
from jax.experimental.pallas import tpu as pltpu
from jax.sharding import Mesh
from jax.sharding import PartitionSpec as P


D = 1024
CANDS = 131072
SESSIONS = 32
STEPS = 3
LANES = 128
PICKS = STEPS * SESSIONS
FLOOR = 0.1
CAND = ("cand_0", "cand_1")
CAND_BLK = ("cand_0", "cand_1", "blk")
FEAT = ("feat_hi", "feat_lo")
EXACT = lax.Precision.HIGHEST
PAIRS = [(t, u) for t in range(STEPS) for u in range(t, STEPS)]
VMEM = pl.BlockSpec(memory_space=pltpu.VMEM)
PARAMS = pltpu.CompilerParams(vmem_limit_bytes=12 << 20)


def share_with(array, axes):
    devices = lax.axis_size(axes)
    copies = jnp.broadcast_to(array, (devices, *array.shape))
    return lax.all_to_all(copies, axes, 0, 0, tiled=True)


def first_step(group, groups):
    return min(group * (CANDS // groups) // (CANDS // STEPS), STEPS - 2)


def winner_rows(embeddings, winners):
    rows_here, width = embeddings.shape
    groups = lax.axis_size(CAND)
    turn = [first_step(g, groups) for g in range(groups)].index(1)
    late = lax.axis_index(CAND) >= turn
    offset = lax.axis_index(CAND_BLK) * rows_here
    by_step = winners.T
    chosen = jnp.where(late, by_step[1:], by_step[:2]).reshape(2 * SESSIONS)
    positions = offset + jnp.arange(rows_here, dtype=jnp.int32)
    onehot = (positions[None, :] == chosen[:, None]).astype(jnp.float32)
    part = jnp.dot(onehot, embeddings, precision=EXACT, preferred_element_type=jnp.float32)
    group_rows = jnp.sum(share_with(part, "blk"), axis=0)
    spread = share_with(group_rows, (*CAND, "feat_lo"))
    spread = spread.reshape(groups, 2, 2, SESSIONS, width)
    low = jnp.sum(spread[:turn], axis=0)
    high = jnp.sum(spread[turn:], axis=0)
    rows = jnp.stack([low[:, 0], low[:, 1] + high[:, 0], high[:, 1]], axis=1)
    return rows.reshape(2, PICKS, width)


def times_rows(left, right):
    return lax.dot_general(
        left, right, (((1,), (1,)), ((), ())), precision=EXACT, preferred_element_type=jnp.float32
    )


def in_rows(tiles):
    at = lax.broadcasted_iota(jnp.int32, (8, LANES), 0)
    tile = jnp.zeros((8, LANES), jnp.float32)
    for row, values in enumerate(tiles):
        tile = jnp.where(at == row, jnp.broadcast_to(values[:1], (8, LANES)), tile)
    return tile


def products_kernel(rows_ref, other_rows_ref, mine_ref, got_ref, out_ref):
    step = lax.broadcasted_iota(jnp.int32, (SESSIONS, LANES), 0)
    lane = lax.broadcasted_iota(jnp.int32, (SESSIONS, LANES), 1)
    rows, other_rows = rows_ref[...], other_rows_ref[...]
    spare = jnp.zeros((LANES - PICKS, LANES), jnp.float32)
    right = jnp.concatenate([rows, spare])
    other_right = jnp.concatenate([other_rows, spare])
    gram = times_rows(rows, right) + times_rows(other_rows, other_right)
    crossed = [
        jnp.sum(
            jnp.where(lane % SESSIONS == step, gram[t * SESSIONS : (t + 1) * SESSIONS], 0.0),
            axis=0,
            keepdims=True,
        )
        for t in range(STEPS)
    ]
    unit = (lax.broadcasted_iota(jnp.int32, (LANES, LANES), 0) == PICKS).astype(jnp.float32)
    for q in range(out_ref.shape[0]):
        norms = []
        for h in range(2):
            at = pl.ds((2 * q + h) * LANES, LANES)
            mine, got = mine_ref[at, :], got_ref[at, :]
            product = times_rows(mine, right) + times_rows(got, other_right)
            product = product + times_rows(mine * mine + got * got, unit)
            turned = product.T
            out_ref[q, pl.ds(h * PICKS, PICKS), :] = turned[:PICKS]
            norms.append(turned[PICKS : PICKS + 1])
        out_ref[q, pl.ds(2 * PICKS, 8), :] = in_rows([*norms, *crossed])


def columns_kernel(parts_ref, out_ref):
    total = parts_ref[0]
    for q in range(1, parts_ref.shape[0]):
        total = total + parts_ref[q]
    total = total * (1.0 / D)
    session = lax.broadcasted_iota(jnp.int32, (SESSIONS, LANES), 0)
    lane = lax.broadcasted_iota(jnp.int32, (SESSIONS, LANES), 1)
    gram = {}
    for t, u in PAIRS:
        row = total[2 * PICKS + 2 + t : 2 * PICKS + 3 + t]
        picked = jnp.where(lane == u * SESSIONS + session, jnp.broadcast_to(row, session.shape), 0.0)
        gram[t, u] = jnp.sum(picked, axis=1, keepdims=True)
    factor, radius = {}, []
    for k in range(STEPS):
        left = gram[k, k]
        for t in range(k):
            left = left - factor[t, k] * factor[t, k]
        radius.append(jnp.sqrt(jnp.maximum(left, FLOOR)))
        for u in range(k + 1, STEPS):
            rest = gram[k, u]
            for t in range(k):
                rest = rest - factor[t, k] * factor[t, u]
            factor[k, u] = rest / radius[k]
    blocks, norms, tops = [], [], [[], []]
    for h in range(2):
        norm = total[2 * PICKS + h : 2 * PICKS + h + 1]
        norms.append(norm)
        gains = jnp.broadcast_to(norm, (SESSIONS, LANES))
        columns = []
        for k in range(STEPS):
            start = h * PICKS + k * SESSIONS
            column = total[start : start + SESSIONS]
            for t in range(k):
                column = column - factor[t, k] * columns[t]
            column = column / radius[k]
            columns.append(column)
            if k < STEPS - 1:
                gains = gains - column * column
                tops[k].append(jnp.max(gains, axis=1, keepdims=True))
        blocks += columns
    first = jnp.max(jnp.maximum(norms[0], norms[1]), axis=1, keepdims=True)
    maxima = [jnp.broadcast_to(first, (SESSIONS, 1))] + [jnp.maximum(*pair) for pair in tops]
    best = jnp.zeros((1, LANES), jnp.float32)
    for k, values in enumerate(maxima):
        placed = jnp.where(lane == k * SESSIONS + session, jnp.broadcast_to(values, session.shape), 0.0)
        best = best + jnp.sum(placed, axis=0, keepdims=True)
    whole = jnp.concatenate([*blocks, in_rows([*norms, best])])
    for f in range(out_ref.shape[0]):
        out_ref[f] = whole


def results_kernel(spread_ref, columns_ref, gains_ref):
    his = spread_ref.shape[0] // 2
    for f in range(2 * his):
        for h in range(2):
            at = pl.ds(((f % 2) * his + f // 2) * 2 * LANES + h * LANES, LANES)
            gains = jnp.broadcast_to(spread_ref[f, pl.ds(2 * PICKS + h, 1), :], (SESSIONS, LANES))
            for k in range(STEPS):
                column = spread_ref[f, pl.ds(h * PICKS + k * SESSIONS, SESSIONS), :]
                columns_ref[k, :, at] = column
                gains = gains - column * column
            gains_ref[:, at] = gains


def selection(embeddings, winners):
    rows_here, _ = embeddings.shape
    his, half = lax.axis_size("feat_hi"), rows_here // 2
    side = lax.axis_index("feat_lo")
    mine = lax.dynamic_slice_in_dim(embeddings, side * half, half)
    other = lax.dynamic_slice_in_dim(embeddings, (1 - side) * half, half)
    got = lax.ppermute(other, "feat_lo", [(0, 1), (1, 0)])
    rows = winner_rows(embeddings, winners)
    own_rows = jnp.where(side == 0, rows[0], rows[1])
    other_rows = jnp.where(side == 0, rows[1], rows[0])
    piece = (2 * PICKS + 8, LANES)
    products = pl.pallas_call(
        products_kernel,
        out_shape=jax.ShapeDtypeStruct((his, *piece), jnp.float32),
        in_specs=[VMEM] * 4,
        out_specs=VMEM,
        cost_estimate=pl.CostEstimate(flops=2 * PICKS * half * 256, bytes_accessed=2 << 20, transcendentals=0),
        compiler_params=PARAMS,
    )(own_rows, other_rows, mine, got)
    parts = lax.all_to_all(products, "feat_hi", 0, 0, tiled=True)
    share = pl.pallas_call(
        columns_kernel,
        out_shape=jax.ShapeDtypeStruct((2 * his, *piece), jnp.float32),
        in_specs=[VMEM],
        out_specs=VMEM,
        cost_estimate=pl.CostEstimate(flops=1 << 20, bytes_accessed=2 << 20, transcendentals=0),
        compiler_params=PARAMS,
    )(parts)
    spread = lax.all_to_all(share, FEAT, 0, 0, tiled=True)
    tops = jnp.max(spread[:, 2 * PICKS + 2, :], axis=0)
    best = share_with(tops.reshape(1, LANES), CAND_BLK).max(axis=(0, 1))
    best = best[:PICKS].reshape(STEPS, SESSIONS).T
    columns, gains = pl.pallas_call(
        results_kernel,
        out_shape=(
            jax.ShapeDtypeStruct((STEPS, SESSIONS, rows_here), jnp.float32),
            jax.ShapeDtypeStruct((SESSIONS, rows_here), jnp.float32),
        ),
        in_specs=[VMEM],
        out_specs=(VMEM, VMEM),
        cost_estimate=pl.CostEstimate(flops=1 << 20, bytes_accessed=2 << 20, transcendentals=0),
        compiler_params=PARAMS,
    )(spread)
    return (columns.transpose(1, 0, 2), gains, best)


def solution(mesh):
    torus = Mesh(
        mesh.devices.reshape(4, 2, mesh.shape["blk"], mesh.shape["feat"] // 2, 2),
        ("cand_0", "cand_1", "blk", "feat_hi", "feat_lo"),
    )
    return jax.shard_map(
        selection,
        mesh=torus,
        in_specs=(P(CAND_BLK, FEAT), P()),
        out_specs=(P(None, None, CAND_BLK), P(None, CAND_BLK), P()),
        check_vma=False,
    )
```

```python
import jax
import jax.numpy as jnp
from jax import lax
from jax.experimental import pallas as pl
from jax.experimental.pallas import tpu as pltpu
from jax.sharding import Mesh
from jax.sharding import PartitionSpec as P


D = 1024
CANDS = 131072
SESSIONS = 32
STEPS = 3
LANES = 128
PICKS = STEPS * SESSIONS
FLOOR = 0.1
CAND = ("cand_0", "cand_1")
CAND_BLK = ("cand_0", "cand_1", "blk")
FEAT = ("feat_hi", "feat_lo")
EXACT = lax.Precision.HIGHEST
PAIRS = [(t, u) for t in range(STEPS) for u in range(t, STEPS)]
VMEM = pl.BlockSpec(memory_space=pltpu.VMEM)
PARAMS = pltpu.CompilerParams(vmem_limit_bytes=12 << 20)


def share_with(array, axes):
    devices = lax.axis_size(axes)
    copies = jnp.broadcast_to(array, (devices, *array.shape))
    return lax.all_to_all(copies, axes, 0, 0, tiled=True)


def first_step(group, groups):
    return min(group * (CANDS // groups) // (CANDS // STEPS), STEPS - 2)


def winner_rows(embeddings, winners):
    rows_here, width = embeddings.shape
    groups = lax.axis_size(CAND)
    turn = [first_step(g, groups) for g in range(groups)].index(1)
    late = lax.axis_index(CAND) >= turn
    offset = lax.axis_index(CAND_BLK) * rows_here
    by_step = winners.T
    chosen = jnp.where(late, by_step[1:], by_step[:2]).reshape(2 * SESSIONS)
    positions = offset + jnp.arange(rows_here, dtype=jnp.int32)
    onehot = (positions[None, :] == chosen[:, None]).astype(jnp.float32)
    part = jnp.dot(onehot, embeddings, precision=EXACT, preferred_element_type=jnp.float32)
    group_rows = jnp.sum(share_with(part, "blk"), axis=0)
    spread = share_with(group_rows, (*CAND, "feat_lo"))
    spread = spread.reshape(groups, 2, 2, SESSIONS, width)
    low = jnp.sum(spread[:turn], axis=0)
    high = jnp.sum(spread[turn:], axis=0)
    rows = jnp.stack([low[:, 0], low[:, 1] + high[:, 0], high[:, 1]], axis=1)
    return rows.reshape(2, PICKS, width)


def times_rows(left, right):
    return lax.dot_general(
        left, right, (((1,), (1,)), ((), ())), precision=EXACT, preferred_element_type=jnp.float32
    )


def in_rows(tiles):
    at = lax.broadcasted_iota(jnp.int32, (8, LANES), 0)
    tile = jnp.zeros((8, LANES), jnp.float32)
    for row, values in enumerate(tiles):
        tile = jnp.where(at == row, jnp.broadcast_to(values[:1], (8, LANES)), tile)
    return tile


def products_kernel(rows_ref, other_rows_ref, mine_ref, got_ref, out_ref):
    step = lax.broadcasted_iota(jnp.int32, (SESSIONS, LANES), 0)
    lane = lax.broadcasted_iota(jnp.int32, (SESSIONS, LANES), 1)
    rows, other_rows = rows_ref[...], other_rows_ref[...]
    spare = jnp.zeros((LANES - PICKS, LANES), jnp.float32)
    right = jnp.concatenate([rows, spare])
    other_right = jnp.concatenate([other_rows, spare])
    gram = times_rows(rows, right) + times_rows(other_rows, other_right)
    crossed = [
        jnp.sum(
            jnp.where(lane % SESSIONS == step, gram[t * SESSIONS : (t + 1) * SESSIONS], 0.0),
            axis=0,
            keepdims=True,
        )
        for t in range(STEPS)
    ]
    unit = (lax.broadcasted_iota(jnp.int32, (LANES, LANES), 0) == PICKS).astype(jnp.float32)
    for q in range(out_ref.shape[0]):
        norms = []
        for h in range(2):
            at = pl.ds((2 * q + h) * LANES, LANES)
            mine, got = mine_ref[at, :], got_ref[at, :]
            product = times_rows(mine, right) + times_rows(got, other_right)
            product = product + times_rows(mine * mine + got * got, unit)
            turned = product.T
            out_ref[q, pl.ds(h * PICKS, PICKS), :] = turned[:PICKS]
            norms.append(turned[PICKS : PICKS + 1])
        out_ref[q, pl.ds(2 * PICKS, 8), :] = in_rows([*norms, *crossed])


def columns_kernel(parts_ref, out_ref):
    total = parts_ref[0]
    for q in range(1, parts_ref.shape[0]):
        total = total + parts_ref[q]
    total = total * (1.0 / D)
    session = lax.broadcasted_iota(jnp.int32, (SESSIONS, LANES), 0)
    lane = lax.broadcasted_iota(jnp.int32, (SESSIONS, LANES), 1)
    gram = {}
    for t, u in PAIRS:
        row = total[2 * PICKS + 2 + t : 2 * PICKS + 3 + t]
        picked = jnp.where(lane == u * SESSIONS + session, jnp.broadcast_to(row, session.shape), 0.0)
        gram[t, u] = jnp.sum(picked, axis=1, keepdims=True)
    factor, radius = {}, []
    for k in range(STEPS):
        left = gram[k, k]
        for t in range(k):
            left = left - factor[t, k] * factor[t, k]
        radius.append(jnp.sqrt(jnp.maximum(left, FLOOR)))
        for u in range(k + 1, STEPS):
            rest = gram[k, u]
            for t in range(k):
                rest = rest - factor[t, k] * factor[t, u]
            factor[k, u] = rest / radius[k]
    blocks, norms, tops = [], [], [[], []]
    for h in range(2):
        norm = total[2 * PICKS + h : 2 * PICKS + h + 1]
        norms.append(norm)
        gains = jnp.broadcast_to(norm, (SESSIONS, LANES))
        columns = []
        for k in range(STEPS):
            start = h * PICKS + k * SESSIONS
            column = total[start : start + SESSIONS]
            for t in range(k):
                column = column - factor[t, k] * columns[t]
            column = column / radius[k]
            columns.append(column)
            if k < STEPS - 1:
                gains = gains - column * column
                tops[k].append(jnp.max(gains, axis=1, keepdims=True))
        blocks += columns
    first = jnp.max(jnp.maximum(norms[0], norms[1]), axis=1, keepdims=True)
    maxima = [jnp.broadcast_to(first, (SESSIONS, 1))] + [jnp.maximum(*pair) for pair in tops]
    best = jnp.zeros((1, LANES), jnp.float32)
    for k, values in enumerate(maxima):
        placed = jnp.where(lane == k * SESSIONS + session, jnp.broadcast_to(values, session.shape), 0.0)
        best = best + jnp.sum(placed, axis=0, keepdims=True)
    whole = jnp.concatenate([*blocks, in_rows([*norms, best])])
    for f in range(out_ref.shape[0]):
        out_ref[f] = whole


def results_kernel(side_ref, own_ref, other_ref, columns_ref, gains_ref):
    his = own_ref.shape[0]
    for side, ref in ((side_ref[0], own_ref), (1 - side_ref[0], other_ref)):
        for q in range(his):
            for h in range(2):
                at = pl.ds(pl.multiple_of((side * his + q) * 2 * LANES + h * LANES, LANES), LANES)
                gains = jnp.broadcast_to(ref[q, pl.ds(2 * PICKS + h, 1), :], (SESSIONS, LANES))
                for k in range(STEPS):
                    column = ref[q, pl.ds(h * PICKS + k * SESSIONS, SESSIONS), :]
                    columns_ref[k, :, at] = column
                    gains = gains - column * column
                gains_ref[:, at] = gains


def selection(embeddings, winners):
    rows_here, _ = embeddings.shape
    his, half = lax.axis_size("feat_hi"), rows_here // 2
    side = lax.axis_index("feat_lo")
    mine = lax.dynamic_slice_in_dim(embeddings, side * half, half)
    away = lax.dynamic_slice_in_dim(embeddings, (1 - side) * half, half)
    got = lax.ppermute(away, "feat_lo", [(0, 1), (1, 0)])
    rows = winner_rows(embeddings, winners)
    own_rows = jnp.where(side == 0, rows[0], rows[1])
    other_rows = jnp.where(side == 0, rows[1], rows[0])
    piece = (2 * PICKS + 8, LANES)
    products = pl.pallas_call(
        products_kernel,
        out_shape=jax.ShapeDtypeStruct((his, *piece), jnp.float32),
        in_specs=[VMEM] * 4,
        out_specs=VMEM,
        cost_estimate=pl.CostEstimate(flops=2 * PICKS * half * 256, bytes_accessed=2 << 20, transcendentals=0),
        compiler_params=PARAMS,
    )(own_rows, other_rows, mine, got)
    parts = lax.all_to_all(products, "feat_hi", 0, 0, tiled=True)
    share = pl.pallas_call(
        columns_kernel,
        out_shape=jax.ShapeDtypeStruct((his, *piece), jnp.float32),
        in_specs=[VMEM],
        out_specs=VMEM,
        cost_estimate=pl.CostEstimate(flops=1 << 20, bytes_accessed=2 << 20, transcendentals=0),
        compiler_params=PARAMS,
    )(parts)
    own = lax.all_to_all(share, "feat_hi", 0, 0, tiled=True)
    other = lax.ppermute(own, "feat_lo", [(0, 1), (1, 0)])
    tops = jnp.max(own[:, 2 * PICKS + 2, :], axis=0)
    best = share_with(tops.reshape(1, LANES), (*CAND_BLK, "feat_lo")).max(axis=(0, 1))
    best = best[:PICKS].reshape(STEPS, SESSIONS).T
    columns, gains = pl.pallas_call(
        results_kernel,
        out_shape=(
            jax.ShapeDtypeStruct((STEPS, SESSIONS, rows_here), jnp.float32),
            jax.ShapeDtypeStruct((SESSIONS, rows_here), jnp.float32),
        ),
        in_specs=[pl.BlockSpec(memory_space=pltpu.SMEM), VMEM, VMEM],
        out_specs=(VMEM, VMEM),
        cost_estimate=pl.CostEstimate(flops=1 << 20, bytes_accessed=2 << 20, transcendentals=0),
        compiler_params=PARAMS,
    )(side.reshape(1), own, other)
    return (columns.transpose(1, 0, 2), gains, best)


def solution(mesh):
    torus = Mesh(
        mesh.devices.reshape(4, 2, mesh.shape["blk"], mesh.shape["feat"] // 2, 2),
        ("cand_0", "cand_1", "blk", "feat_hi", "feat_lo"),
    )
    return jax.shard_map(
        selection,
        mesh=torus,
        in_specs=(P(CAND_BLK, FEAT), P()),
        out_specs=(P(None, None, CAND_BLK), P(None, CAND_BLK), P()),
        check_vma=False,
    )
```

```python
import functools

import jax
import jax.numpy as jnp
from jax import lax
from jax.experimental import pallas as pl
from jax.experimental.pallas import tpu as pltpu
from jax.sharding import Mesh
from jax.sharding import PartitionSpec as P


D = 1024
CANDS = 131072
SESSIONS = 32
STEPS = 3
LANES = 128
PICKS = STEPS * SESSIONS
FLOOR = 0.1
CAND = ("cand_0", "cand_1")
CAND_BLK = ("cand_0", "cand_1", "blk")
FEAT = ("feat_hi", "feat_lo")
EXACT = lax.Precision.HIGHEST
PAIRS = [(t, u) for t in range(STEPS) for u in range(t, STEPS)]
VMEM = pl.BlockSpec(memory_space=pltpu.VMEM)
HBM = pl.BlockSpec(memory_space=pl.ANY)
SMEM = pl.BlockSpec(memory_space=pltpu.SMEM)
PARAMS = pltpu.CompilerParams(vmem_limit_bytes=12 << 20)


def share_with(array, axes):
    devices = lax.axis_size(axes)
    copies = jnp.broadcast_to(array, (devices, *array.shape))
    return lax.all_to_all(copies, axes, 0, 0, tiled=True)


def first_step(group, groups):
    return min(group * (CANDS // groups) // (CANDS // STEPS), STEPS - 2)


def picks_kernel(turn, winners_hbm, embeddings_hbm, out_ref, winners_ref, embeddings_ref, sems):
    fetch_rows = pltpu.make_async_copy(embeddings_hbm, embeddings_ref, sems.at[0])
    fetch_winners = pltpu.make_async_copy(winners_hbm, winners_ref, sems.at[1])
    fetch_rows.start()
    fetch_winners.start()
    fetch_winners.wait()
    fetch_rows.wait()
    rows_here = embeddings_ref.shape[0]
    first = (lax.axis_index(CAND) >= turn).astype(jnp.int32)
    offset = lax.axis_index(CAND_BLK) * rows_here
    at = lax.broadcasted_iota(jnp.int32, (8, LANES), 0)
    for start in range(0, 2 * SESSIONS, 8):
        tile = jnp.zeros((8, LANES), jnp.float32)
        for row in range(8):
            step, session = divmod(start + row, SESSIONS)
            here = winners_ref[first + step, session] - offset
            held = jnp.logical_and(here >= 0, here < rows_here)
            values = embeddings_ref[pl.ds(jnp.clip(here, 0, rows_here - 1), 1), :]
            wanted = jnp.logical_and(at == row, held)
            tile = jnp.where(wanted, jnp.broadcast_to(values, (8, LANES)), tile)
        for copy in range(out_ref.shape[0]):
            out_ref[copy, pl.ds(start, 8), :] = tile


def winner_rows(embeddings, winners):
    rows_here, width = embeddings.shape
    groups = lax.axis_size(CAND)
    turn = [first_step(g, groups) for g in range(groups)].index(1)
    blks = lax.axis_size("blk")
    part = pl.pallas_call(
        functools.partial(picks_kernel, turn),
        out_shape=jax.ShapeDtypeStruct((blks, 2 * SESSIONS, width), jnp.float32),
        in_specs=[HBM, HBM],
        out_specs=VMEM,
        scratch_shapes=[
            pltpu.SMEM((STEPS, SESSIONS), jnp.int32),
            pltpu.VMEM((rows_here, width), jnp.float32),
            pltpu.SemaphoreType.DMA((2,)),
        ],
        cost_estimate=pl.CostEstimate(flops=1 << 20, bytes_accessed=1 << 20, transcendentals=0),
    )(winners.T, embeddings)
    part = lax.all_to_all(part, "blk", 0, 0, tiled=True)
    group_rows = jnp.sum(part, axis=0)
    spread = share_with(group_rows, (*CAND, "feat_lo"))
    spread = spread.reshape(groups, 2, 2, SESSIONS, width)
    low = jnp.sum(spread[:turn], axis=0)
    high = jnp.sum(spread[turn:], axis=0)
    rows = jnp.stack([low[:, 0], low[:, 1] + high[:, 0], high[:, 1]], axis=1)
    return rows.reshape(2, PICKS, width)


def times_rows(left, right):
    return lax.dot_general(
        left, right, (((1,), (1,)), ((), ())), precision=EXACT, preferred_element_type=jnp.float32
    )


def in_rows(tiles):
    at = lax.broadcasted_iota(jnp.int32, (8, LANES), 0)
    tile = jnp.zeros((8, LANES), jnp.float32)
    for row, values in enumerate(tiles):
        tile = jnp.where(at == row, jnp.broadcast_to(values[:1], (8, LANES)), tile)
    return tile


def products_kernel(side_ref, rows_ref, mine_ref, got_ref, out_ref):
    session = lax.broadcasted_iota(jnp.int32, (SESSIONS, LANES), 0)
    lane = lax.broadcasted_iota(jnp.int32, (SESSIONS, LANES), 1)
    rows = jnp.concatenate([rows_ref[side_ref[0]], rows_ref[1 - side_ref[0]]], axis=1)
    right = jnp.concatenate([rows, jnp.zeros((LANES - PICKS, 2 * LANES), jnp.float32)])
    gram = times_rows(rows, right)
    crossed = [
        jnp.sum(
            jnp.where(lane % SESSIONS == session, gram[t * SESSIONS : (t + 1) * SESSIONS], 0.0),
            axis=0,
            keepdims=True,
        )
        for t in range(STEPS)
    ]
    norm_lane = lax.broadcasted_iota(jnp.int32, (2 * LANES, LANES), 1) == PICKS
    for q in range(out_ref.shape[0]):
        at = pl.ds(q * 2 * LANES, 2 * LANES)
        mine, got = mine_ref[at, :], got_ref[at, :]
        product = times_rows(jnp.concatenate([mine, got], axis=1), right)
        norm = jnp.sum(mine * mine + got * got, axis=1, keepdims=True)
        product = jnp.where(norm_lane, norm, product)
        norms = []
        for h in range(2):
            turned = product[h * LANES : (h + 1) * LANES].T
            out_ref[q, pl.ds(h * PICKS, PICKS), :] = turned[:PICKS]
            norms.append(turned[PICKS : PICKS + 1])
        out_ref[q, pl.ds(2 * PICKS, 8), :] = in_rows([*norms, *crossed])


def columns_kernel(parts_ref, out_ref):
    total = parts_ref[0]
    for q in range(1, parts_ref.shape[0]):
        total = total + parts_ref[q]
    total = total * (1.0 / D)
    session = lax.broadcasted_iota(jnp.int32, (SESSIONS, LANES), 0)
    lane = lax.broadcasted_iota(jnp.int32, (SESSIONS, LANES), 1)
    gram = {}
    for t, u in PAIRS:
        row = total[2 * PICKS + 2 + t : 2 * PICKS + 3 + t]
        picked = jnp.where(lane == u * SESSIONS + session, jnp.broadcast_to(row, session.shape), 0.0)
        gram[t, u] = jnp.sum(picked, axis=1, keepdims=True)
    factor, radius = {}, []
    for k in range(STEPS):
        left = gram[k, k]
        for t in range(k):
            left = left - factor[t, k] * factor[t, k]
        radius.append(jnp.sqrt(jnp.maximum(left, FLOOR)))
        for u in range(k + 1, STEPS):
            rest = gram[k, u]
            for t in range(k):
                rest = rest - factor[t, k] * factor[t, u]
            factor[k, u] = rest / radius[k]
    blocks, norms, tops = [], [], [[], []]
    for h in range(2):
        norm = total[2 * PICKS + h : 2 * PICKS + h + 1]
        norms.append(norm)
        gains = jnp.broadcast_to(norm, (SESSIONS, LANES))
        columns = []
        for k in range(STEPS):
            start = h * PICKS + k * SESSIONS
            column = total[start : start + SESSIONS]
            for t in range(k):
                column = column - factor[t, k] * columns[t]
            column = column / radius[k]
            columns.append(column)
            if k < STEPS - 1:
                gains = gains - column * column
                tops[k].append(jnp.max(gains, axis=1, keepdims=True))
        blocks += columns
    first = jnp.max(jnp.maximum(norms[0], norms[1]), axis=1, keepdims=True)
    maxima = [jnp.broadcast_to(first, (SESSIONS, 1))] + [jnp.maximum(*pair) for pair in tops]
    best = jnp.zeros((1, LANES), jnp.float32)
    for k, values in enumerate(maxima):
        placed = jnp.where(lane == k * SESSIONS + session, jnp.broadcast_to(values, session.shape), 0.0)
        best = best + jnp.sum(placed, axis=0, keepdims=True)
    whole = jnp.concatenate([*blocks, in_rows([*norms, best])])
    for f in range(out_ref.shape[0]):
        out_ref[f] = whole


def results_kernel(side_ref, own_ref, other_ref, columns_ref, gains_ref):
    his = own_ref.shape[0]
    for side, ref in ((side_ref[0], own_ref), (1 - side_ref[0], other_ref)):
        for q in range(his):
            for h in range(2):
                at = pl.ds(pl.multiple_of((side * his + q) * 2 * LANES + h * LANES, LANES), LANES)
                gains = jnp.broadcast_to(ref[q, pl.ds(2 * PICKS + h, 1), :], (SESSIONS, LANES))
                for k in range(STEPS):
                    column = ref[q, pl.ds(h * PICKS + k * SESSIONS, SESSIONS), :]
                    columns_ref[k, :, at] = column
                    gains = gains - column * column
                gains_ref[:, at] = gains


def selection(embeddings, winners):
    rows_here, _ = embeddings.shape
    his, half = lax.axis_size("feat_hi"), rows_here // 2
    side = lax.axis_index("feat_lo")
    mine = lax.dynamic_slice_in_dim(embeddings, side * half, half)
    away = lax.dynamic_slice_in_dim(embeddings, (1 - side) * half, half)
    got = lax.ppermute(away, "feat_lo", [(0, 1), (1, 0)])
    rows = winner_rows(embeddings, winners)
    piece = (2 * PICKS + 8, LANES)
    products = pl.pallas_call(
        products_kernel,
        out_shape=jax.ShapeDtypeStruct((his, *piece), jnp.float32),
        in_specs=[SMEM, VMEM, VMEM, VMEM],
        out_specs=VMEM,
        cost_estimate=pl.CostEstimate(flops=2 * PICKS * half * 256, bytes_accessed=2 << 20, transcendentals=0),
        compiler_params=PARAMS,
    )(side.reshape(1), rows, mine, got)
    parts = lax.all_to_all(products, "feat_hi", 0, 0, tiled=True)
    share = pl.pallas_call(
        columns_kernel,
        out_shape=jax.ShapeDtypeStruct((his, *piece), jnp.float32),
        in_specs=[VMEM],
        out_specs=VMEM,
        cost_estimate=pl.CostEstimate(flops=1 << 20, bytes_accessed=2 << 20, transcendentals=0),
        compiler_params=PARAMS,
    )(parts)
    own = lax.all_to_all(share, "feat_hi", 0, 0, tiled=True)
    other = lax.ppermute(own, "feat_lo", [(0, 1), (1, 0)])
    tops = jnp.max(own[:, 2 * PICKS + 2, :], axis=0)
    best = share_with(tops.reshape(1, LANES), (*CAND_BLK, "feat_lo")).max(axis=(0, 1))
    best = best[:PICKS].reshape(STEPS, SESSIONS).T
    columns, gains = pl.pallas_call(
        results_kernel,
        out_shape=(
            jax.ShapeDtypeStruct((STEPS, SESSIONS, rows_here), jnp.float32),
            jax.ShapeDtypeStruct((SESSIONS, rows_here), jnp.float32),
        ),
        in_specs=[SMEM, VMEM, VMEM],
        out_specs=(VMEM, VMEM),
        cost_estimate=pl.CostEstimate(flops=1 << 20, bytes_accessed=2 << 20, transcendentals=0),
        compiler_params=PARAMS,
    )(side.reshape(1), own, other)
    return (columns.transpose(1, 0, 2), gains, best)


def solution(mesh):
    torus = Mesh(
        mesh.devices.reshape(4, 2, mesh.shape["blk"], mesh.shape["feat"] // 2, 2),
        ("cand_0", "cand_1", "blk", "feat_hi", "feat_lo"),
    )
    return jax.shard_map(
        selection,
        mesh=torus,
        in_specs=(P(CAND_BLK, FEAT), P()),
        out_specs=(P(None, None, CAND_BLK), P(None, CAND_BLK), P()),
        check_vma=False,
    )
```

```python
import functools

import jax
import jax.numpy as jnp
from jax import lax
from jax.experimental import pallas as pl
from jax.experimental.pallas import tpu as pltpu
from jax.sharding import Mesh
from jax.sharding import PartitionSpec as P


D = 1024
CANDS = 131072
SESSIONS = 32
STEPS = 3
LANES = 128
PICKS = STEPS * SESSIONS
FLOOR = 0.1
CAND = ("cand_0", "cand_1")
CAND_BLK = ("cand_0", "cand_1", "blk")
FEAT = ("feat_hi", "feat_lo")
EXACT = lax.Precision.HIGHEST
PAIRS = [(t, u) for t in range(STEPS) for u in range(t, STEPS)]
VMEM = pl.BlockSpec(memory_space=pltpu.VMEM)
HBM = pl.BlockSpec(memory_space=pl.ANY)
SMEM = pl.BlockSpec(memory_space=pltpu.SMEM)
PARAMS = pltpu.CompilerParams(vmem_limit_bytes=12 << 20)


def share_with(array, axes):
    devices = lax.axis_size(axes)
    copies = jnp.broadcast_to(array, (devices, *array.shape))
    return lax.all_to_all(copies, axes, 0, 0, tiled=True)


def first_step(group, groups):
    return min(group * (CANDS // groups) // (CANDS // STEPS), STEPS - 2)


def picks_kernel(turn, winners_hbm, embeddings_hbm, out_ref, winners_ref, embeddings_ref, sems):
    fetch_rows = pltpu.make_async_copy(embeddings_hbm, embeddings_ref, sems.at[0])
    fetch_winners = pltpu.make_async_copy(winners_hbm, winners_ref, sems.at[1])
    fetch_rows.start()
    fetch_winners.start()
    fetch_winners.wait()
    fetch_rows.wait()
    rows_here = embeddings_ref.shape[0]
    first = (lax.axis_index("cand_0") >= turn).astype(jnp.int32)
    offset = lax.axis_index(CAND_BLK) * rows_here
    at = lax.broadcasted_iota(jnp.int32, (8, LANES), 0)
    blks = out_ref.shape[0] // 2
    for step in range(2):
        for start in range(0, SESSIONS, 8):
            tile = jnp.zeros((8, LANES), jnp.float32)
            for row in range(8):
                here = winners_ref[first + step, start + row] - offset
                held = jnp.logical_and(here >= 0, here < rows_here)
                values = embeddings_ref[pl.ds(jnp.clip(here, 0, rows_here - 1), 1), :]
                wanted = jnp.logical_and(at == row, held)
                tile = jnp.where(wanted, jnp.broadcast_to(values, (8, LANES)), tile)
            for copy in range(blks):
                out_ref[step * blks + copy, pl.ds(start, 8), :] = tile


def winner_rows(embeddings, winners):
    rows_here, width = embeddings.shape
    groups = lax.axis_size("cand_0")
    turn = [first_step(g, groups) for g in range(groups)].index(1)
    blks = lax.axis_size("blk")
    part = pl.pallas_call(
        functools.partial(picks_kernel, turn),
        out_shape=jax.ShapeDtypeStruct((2 * blks, SESSIONS, width), jnp.float32),
        in_specs=[HBM, HBM],
        out_specs=VMEM,
        scratch_shapes=[
            pltpu.SMEM((STEPS, SESSIONS), jnp.int32),
            pltpu.VMEM((rows_here, width), jnp.float32),
            pltpu.SemaphoreType.DMA((2,)),
        ],
        cost_estimate=pl.CostEstimate(flops=1 << 20, bytes_accessed=1 << 20, transcendentals=0),
    )(winners.T, embeddings)
    part = lax.all_to_all(part, ("cand_1", "blk"), 0, 0, tiled=True)
    group_rows = jnp.sum(part, axis=0)
    spread = share_with(group_rows, (*CAND, "feat_lo"))
    spread = spread.reshape(groups, 2, 2, SESSIONS, width)
    low = jnp.sum(spread[:turn], axis=0)
    high = jnp.sum(spread[turn:], axis=0)
    rows = jnp.stack([low[0], low[1] + high[0], high[1]], axis=1)
    return rows.reshape(2, PICKS, width)


def times_rows(left, right):
    return lax.dot_general(
        left, right, (((1,), (1,)), ((), ())), precision=EXACT, preferred_element_type=jnp.float32
    )


def in_rows(tiles):
    at = lax.broadcasted_iota(jnp.int32, (8, LANES), 0)
    tile = jnp.zeros((8, LANES), jnp.float32)
    for row, values in enumerate(tiles):
        tile = jnp.where(at == row, jnp.broadcast_to(values[:1], (8, LANES)), tile)
    return tile


def products_kernel(side_ref, rows_ref, mine_ref, got_ref, out_ref):
    session = lax.broadcasted_iota(jnp.int32, (SESSIONS, LANES), 0)
    lane = lax.broadcasted_iota(jnp.int32, (SESSIONS, LANES), 1)
    rows = jnp.concatenate([rows_ref[side_ref[0]], rows_ref[1 - side_ref[0]]], axis=1)
    right = jnp.concatenate([rows, jnp.zeros((LANES - PICKS, 2 * LANES), jnp.float32)])
    gram = times_rows(rows, right)
    crossed = [
        jnp.sum(
            jnp.where(lane % SESSIONS == session, gram[t * SESSIONS : (t + 1) * SESSIONS], 0.0),
            axis=0,
            keepdims=True,
        )
        for t in range(STEPS)
    ]
    norm_lane = lax.broadcasted_iota(jnp.int32, (2 * LANES, LANES), 1) == PICKS
    for q in range(out_ref.shape[0]):
        at = pl.ds(q * 2 * LANES, 2 * LANES)
        mine, got = mine_ref[at, :], got_ref[at, :]
        product = times_rows(jnp.concatenate([mine, got], axis=1), right)
        norm = jnp.sum(mine * mine + got * got, axis=1, keepdims=True)
        product = jnp.where(norm_lane, norm, product)
        norms = []
        for h in range(2):
            turned = product[h * LANES : (h + 1) * LANES].T
            out_ref[q, pl.ds(h * PICKS, PICKS), :] = turned[:PICKS]
            norms.append(turned[PICKS : PICKS + 1])
        out_ref[q, pl.ds(2 * PICKS, 8), :] = in_rows([*norms, *crossed])


def columns_kernel(parts_ref, out_ref):
    total = parts_ref[0]
    for q in range(1, parts_ref.shape[0]):
        total = total + parts_ref[q]
    total = total * (1.0 / D)
    session = lax.broadcasted_iota(jnp.int32, (SESSIONS, LANES), 0)
    lane = lax.broadcasted_iota(jnp.int32, (SESSIONS, LANES), 1)
    gram = {}
    for t, u in PAIRS:
        row = total[2 * PICKS + 2 + t : 2 * PICKS + 3 + t]
        picked = jnp.where(lane == u * SESSIONS + session, jnp.broadcast_to(row, session.shape), 0.0)
        gram[t, u] = jnp.sum(picked, axis=1, keepdims=True)
    factor, radius = {}, []
    for k in range(STEPS):
        left = gram[k, k]
        for t in range(k):
            left = left - factor[t, k] * factor[t, k]
        radius.append(jnp.sqrt(jnp.maximum(left, FLOOR)))
        for u in range(k + 1, STEPS):
            rest = gram[k, u]
            for t in range(k):
                rest = rest - factor[t, k] * factor[t, u]
            factor[k, u] = rest / radius[k]
    blocks, norms, tops = [], [], [[], []]
    for h in range(2):
        norm = total[2 * PICKS + h : 2 * PICKS + h + 1]
        norms.append(norm)
        gains = jnp.broadcast_to(norm, (SESSIONS, LANES))
        columns = []
        for k in range(STEPS):
            start = h * PICKS + k * SESSIONS
            column = total[start : start + SESSIONS]
            for t in range(k):
                column = column - factor[t, k] * columns[t]
            column = column / radius[k]
            columns.append(column)
            if k < STEPS - 1:
                gains = gains - column * column
                tops[k].append(jnp.max(gains, axis=1, keepdims=True))
        blocks += columns
    first = jnp.max(jnp.maximum(norms[0], norms[1]), axis=1, keepdims=True)
    maxima = [jnp.broadcast_to(first, (SESSIONS, 1))] + [jnp.maximum(*pair) for pair in tops]
    best = jnp.zeros((1, LANES), jnp.float32)
    for k, values in enumerate(maxima):
        placed = jnp.where(lane == k * SESSIONS + session, jnp.broadcast_to(values, session.shape), 0.0)
        best = best + jnp.sum(placed, axis=0, keepdims=True)
    whole = jnp.concatenate([*blocks, in_rows([*norms, best])])
    for f in range(out_ref.shape[0]):
        out_ref[f] = whole


def results_kernel(side_ref, own_ref, other_ref, columns_ref, gains_ref):
    his = own_ref.shape[0]
    for side, ref in ((side_ref[0], own_ref), (1 - side_ref[0], other_ref)):
        for q in range(his):
            for h in range(2):
                at = pl.ds(pl.multiple_of((side * his + q) * 2 * LANES + h * LANES, LANES), LANES)
                gains = jnp.broadcast_to(ref[q, pl.ds(2 * PICKS + h, 1), :], (SESSIONS, LANES))
                for k in range(STEPS):
                    column = ref[q, pl.ds(h * PICKS + k * SESSIONS, SESSIONS), :]
                    columns_ref[k, :, at] = column
                    gains = gains - column * column
                gains_ref[:, at] = gains


def selection(embeddings, winners):
    rows_here, _ = embeddings.shape
    his, half = lax.axis_size("feat_hi"), rows_here // 2
    side = lax.axis_index("feat_lo")
    mine = lax.dynamic_slice_in_dim(embeddings, side * half, half)
    away = lax.dynamic_slice_in_dim(embeddings, (1 - side) * half, half)
    got = lax.ppermute(away, "feat_lo", [(0, 1), (1, 0)])
    rows = winner_rows(embeddings, winners)
    piece = (2 * PICKS + 8, LANES)
    products = pl.pallas_call(
        products_kernel,
        out_shape=jax.ShapeDtypeStruct((his, *piece), jnp.float32),
        in_specs=[SMEM, VMEM, VMEM, VMEM],
        out_specs=VMEM,
        cost_estimate=pl.CostEstimate(flops=2 * PICKS * half * 256, bytes_accessed=2 << 20, transcendentals=0),
        compiler_params=PARAMS,
    )(side.reshape(1), rows, mine, got)
    parts = lax.all_to_all(products, "feat_hi", 0, 0, tiled=True)
    share = pl.pallas_call(
        columns_kernel,
        out_shape=jax.ShapeDtypeStruct((his, *piece), jnp.float32),
        in_specs=[VMEM],
        out_specs=VMEM,
        cost_estimate=pl.CostEstimate(flops=1 << 20, bytes_accessed=2 << 20, transcendentals=0),
        compiler_params=PARAMS,
    )(parts)
    own = lax.all_to_all(share, "feat_hi", 0, 0, tiled=True)
    other = lax.ppermute(own, "feat_lo", [(0, 1), (1, 0)])
    tops = jnp.max(own[:, 2 * PICKS + 2, :], axis=0)
    best = share_with(tops.reshape(1, LANES), (*CAND_BLK, "feat_lo")).max(axis=(0, 1))
    best = best[:PICKS].reshape(STEPS, SESSIONS).T
    columns, gains = pl.pallas_call(
        results_kernel,
        out_shape=(
            jax.ShapeDtypeStruct((STEPS, SESSIONS, rows_here), jnp.float32),
            jax.ShapeDtypeStruct((SESSIONS, rows_here), jnp.float32),
        ),
        in_specs=[SMEM, VMEM, VMEM],
        out_specs=(VMEM, VMEM),
        cost_estimate=pl.CostEstimate(flops=1 << 20, bytes_accessed=2 << 20, transcendentals=0),
        compiler_params=PARAMS,
    )(side.reshape(1), own, other)
    return (columns.transpose(1, 0, 2), gains, best)


def solution(mesh):
    torus = Mesh(
        mesh.devices.reshape(4, 2, mesh.shape["blk"], mesh.shape["feat"] // 2, 2),
        ("cand_0", "cand_1", "blk", "feat_hi", "feat_lo"),
    )
    return jax.shard_map(
        selection,
        mesh=torus,
        in_specs=(P(CAND_BLK, FEAT), P()),
        out_specs=(P(None, None, CAND_BLK), P(None, CAND_BLK), P()),
        check_vma=False,
    )
```
